32 devices in a mesh: dp: 2 (over x), ep: 16 (over z, y, core).
Axes of the slice: x: 2, y: 2, z: 4, core: 2. Of those that a mesh axis runs over, the one named last changes fastest.
Arguments:
- h0: bfloat16 [32, 1024, 2048], P(('dp', 'ep')), parts along dimension 0
- idx: int32 [32, 1024, 6], P(('dp', 'ep')), parts along dimension 0
- slot: int32 [32, 1024, 6], P(('dp', 'ep')), parts along dimension 0
- ln_attn: bfloat16 [2048], replicated
- wq: bfloat16 [2048, 2048], replicated
- wk: bfloat16 [2048, 2048], replicated
- wv: bfloat16 [2048, 2048], replicated
- wo: bfloat16 [2048, 2048], replicated
- ln_ffn: bfloat16 [2048], replicated
- ws1: bfloat16 [2048, 2816], replicated
- ws3: bfloat16 [2048, 2816], replicated
- ws2: bfloat16 [2816, 2048], replicated
- ln_moe: bfloat16 [2048], replicated
- wr: bfloat16 [2048, 64], replicated
- ue1: bfloat16 [64, 2048, 1408], P('ep')
- ue3: bfloat16 [64, 2048, 1408], P('ep')
- ue2: bfloat16 [64, 1408, 2048], P('ep')
Outputs:
- output: bfloat16 [32, 1024, 2048], P(('dp', 'ep')), parts along dimension 0
There are 2 independent parts. The reference program is written for one: setup_inputs(seed, part) draws one part's arguments, and reference() takes and returns one part's arrays. A program takes and returns all parts, laid end to end along the dimension named above; an argument that names none is the same for every part.
All inputs are finite; a program needn't handle non-finite values.
Results may differ from the reference program's by a relative error of at most 0.0102627.
Values are sent between devices in bfloat16 or wider.
A program may use at most 1 GiB of HBM per device.

```python
import jax
import jax.numpy as jnp
from jax import lax

D = 2048
HEADS = 16
HEAD = 128
EXPERTS = 64
TOP = 6
FE = 1408
FS = 2816
SEQ = 1024
SEQS = 1
G = 16
CAP = 192

T = SEQS * SEQ
EPS = 1e-6


def _dot(a, b):
    return jnp.dot(a, b, preferred_element_type=jnp.float32)


def _rms(x, w):
    xf = x.astype(jnp.float32)
    r = lax.rsqrt(jnp.mean(xf * xf, axis=-1, keepdims=True) + EPS)
    return (xf * r * w.astype(jnp.float32)).astype(jnp.bfloat16)


def _rope(x):
    half = HEAD // 2
    freq = 10000.0 ** (-jnp.arange(half, dtype=jnp.float32) / half)
    ang = jnp.arange(SEQ, dtype=jnp.float32)[:, None] * freq[None, :]
    c = jnp.cos(ang)[:, None, :]
    s = jnp.sin(ang)[:, None, :]
    x1, x2 = x[..., :half], x[..., half:]
    return jnp.concatenate([x1 * c - x2 * s, x2 * c + x1 * s], axis=-1)


def _normal(key, shape, scale):
    return (jax.random.normal(key, shape, jnp.float32) * scale).astype(jnp.bfloat16)


def _scale(key):
    return jax.random.uniform(key, (D,), jnp.float32, 0.8, 1.2).astype(jnp.bfloat16)


def _expert_weight(weight_key):
    levels = jnp.sum(jax.random.randint(weight_key, (9, EXPERTS), 0, 10, jnp.int32), axis=0)
    hot_bias = 12 * (jnp.arange(EXPERTS) < EXPERTS // G).astype(jnp.int32)
    quarter = jnp.maximum(levels + hot_bias - 16, 0)
    return jnp.left_shift(4 + quarter % 4, quarter // 4).astype(jnp.int32)


def _route(route_key, weight):
    draw_rows = jax.random.bits(route_key, (T, TOP), jnp.uint32)

    def step(counts, draw_row):
        open_weight = jnp.where(counts < CAP, weight, 0).astype(jnp.int32)
        picked_list = []
        for choice in range(TOP):
            cumulative = jnp.cumsum(open_weight)
            total_weight = cumulative[-1].astype(jnp.uint32)
            target_val = (draw_row[choice] % total_weight).astype(jnp.int32)
            pick_id = jnp.searchsorted(cumulative, target_val, side='right').astype(jnp.int32)
            picked_list.append(pick_id)
            open_weight = open_weight.at[pick_id].set(0)
        chosen = jnp.stack(picked_list)
        return counts.at[chosen].add(1), (chosen, counts[chosen])

    _, (chosen, slots) = lax.scan(step, jnp.zeros((EXPERTS,), jnp.int32), draw_rows)
    return chosen.astype(jnp.int32), slots.astype(jnp.int32)


def setup_inputs(seed: int = 0, part: int = 0) -> dict:
    key = jax.random.PRNGKey(seed)
    kh, kr = jax.random.split(jax.random.fold_in(key, part))
    ks = jax.random.split(key, 15)
    hd = HEADS * HEAD
    expert_weight = _expert_weight(jax.random.fold_in(ks[14], 7))
    idx, slot = jax.vmap(lambda k: _route(k, expert_weight))(jax.random.split(kr, G))
    return {
        'h0': _normal(kh, (G * SEQS, SEQ, D), 1.0),
        'idx': idx.reshape(G * SEQS, SEQ, TOP),
        'slot': slot.reshape(G * SEQS, SEQ, TOP),
        'ln_attn': _scale(ks[0]),
        'wq': _normal(ks[1], (D, hd), 1.5 * D ** -0.5),
        'wk': _normal(ks[2], (D, hd), 1.5 * D ** -0.5),
        'wv': _normal(ks[3], (D, hd), D ** -0.5),
        'wo': _normal(ks[4], (hd, D), hd ** -0.5),
        'ln_ffn': _scale(ks[5]),
        'ws1': _normal(ks[6], (D, FS), D ** -0.5),
        'ws3': _normal(ks[7], (D, FS), D ** -0.5),
        'ws2': _normal(ks[8], (FS, D), FS ** -0.5),
        'ln_moe': _scale(ks[9]),
        'wr': _normal(ks[10], (D, EXPERTS), 1.5 * D ** -0.5),
        'ue1': _normal(ks[11], (EXPERTS, D, FE), D ** -0.5),
        'ue3': _normal(ks[12], (EXPERTS, D, FE), D ** -0.5),
        'ue2': _normal(ks[13], (EXPERTS, FE, D), 2.0 * FE ** -0.5),
    }


def reference(h0, idx, slot, ln_attn, wq, wk, wv, wo, ln_ffn, ws1, ws3, ws2, ln_moe, wr, ue1, ue3, ue2):
    nb = h0.shape[0]
    n = nb * SEQ
    x1 = _rms(h0, ln_attn)
    causal = jnp.arange(SEQ)[:, None] >= jnp.arange(SEQ)[None, :]

    def attn(xs):
        q = _rope(_dot(xs, wq).reshape(SEQ, HEADS, HEAD)).astype(jnp.bfloat16)
        k = _rope(_dot(xs, wk).reshape(SEQ, HEADS, HEAD)).astype(jnp.bfloat16)
        v = _dot(xs, wv).astype(jnp.bfloat16).reshape(SEQ, HEADS, HEAD)
        s = jnp.einsum('qhe,khe->hqk', q.astype(jnp.float32), k.astype(jnp.float32)) * HEAD ** -0.5
        p = jax.nn.softmax(jnp.where(causal[None], s, -1e30), axis=-1).astype(jnp.bfloat16)
        o = jnp.einsum('hqk,khe->qhe', p.astype(jnp.float32), v.astype(jnp.float32))
        return o.astype(jnp.bfloat16).reshape(SEQ, HEADS * HEAD)

    o = lax.map(attn, x1).reshape(n, HEADS * HEAD)
    h = h0.reshape(n, D)
    a = (h.astype(jnp.float32) + _dot(o, wo)).astype(jnp.bfloat16)
    x2 = _rms(a, ln_ffn)
    hs = (jax.nn.silu(_dot(x2, ws1)) * _dot(x2, ws3)).astype(jnp.bfloat16)
    f = _dot(hs, ws2)

    u = _rms(h, ln_moe)
    gi = idx.reshape(n, TOP)
    sl = slot.reshape(n, TOP)
    g = jax.nn.softmax(jnp.take_along_axis(_dot(u, wr), gi, axis=1), axis=-1)
    dev = jnp.arange(n, dtype=jnp.int32) // T
    pos = gi * (G * CAP) + dev[:, None] * CAP + sl
    src = jnp.full((EXPERTS * G * CAP,), n, jnp.int32).at[pos.reshape(-1)].set(
        jnp.arange(n * TOP, dtype=jnp.int32) // TOP)
    u_pad = jnp.concatenate([u, jnp.zeros((1, D), jnp.bfloat16)], axis=0)
    buf = u_pad[src].reshape(EXPERTS, G * CAP, D)

    def expert(args):
        x, w1, w3, w2 = args
        he = (jax.nn.silu(_dot(x, w1)) * _dot(x, w3)).astype(jnp.bfloat16)
        return _dot(he, w2).astype(jnp.bfloat16)

    y = lax.map(expert, (buf, ue1, ue3, ue2)).reshape(EXPERTS * G * CAP, D)
    m = jnp.sum(g[:, :, None] * y[pos].astype(jnp.float32), axis=1)
    out = a.astype(jnp.float32) + f + m
    return out.astype(jnp.bfloat16).reshape(nb, SEQ, D)
```

```python
import jax
import jax.numpy as jnp
from jax import lax
from jax.sharding import PartitionSpec as P

HEAD = 128
EPS = 1e-6
CAP_FACTOR = 2


def _mm(form, a, b):
    return jnp.einsum(form, a, b, preferred_element_type=jnp.float32)


def _rms(x, w):
    xf = x.astype(jnp.float32)
    r = lax.rsqrt(jnp.mean(xf * xf, axis=-1, keepdims=True) + EPS)
    return (xf * r * w.astype(jnp.float32)).astype(jnp.bfloat16)


def _rope(x):
    s, half = x.shape[1], x.shape[-1] // 2
    freq = 10000.0 ** (-jnp.arange(half, dtype=jnp.float32) / half)
    ang = jnp.arange(s, dtype=jnp.float32)[:, None] * freq[None, :]
    c = jnp.cos(ang)[None, :, None, :]
    sn = jnp.sin(ang)[None, :, None, :]
    x1, x2 = x[..., :half], x[..., half:]
    return jnp.concatenate([x1 * c - x2 * sn, x2 * c + x1 * sn], axis=-1)


def _dense(h0, ln_attn, wq, wk, wv, wo, ln_ffn, ws1, ws3, ws2):
    b, s, _ = h0.shape
    nh = wq.shape[1] // HEAD
    x1 = _rms(h0, ln_attn)
    q = _rope(_mm('bsd,de->bse', x1, wq).reshape(b, s, nh, HEAD)).astype(jnp.bfloat16)
    k = _rope(_mm('bsd,de->bse', x1, wk).reshape(b, s, nh, HEAD)).astype(jnp.bfloat16)
    v = _mm('bsd,de->bse', x1, wv).astype(jnp.bfloat16).reshape(b, s, nh, HEAD)
    sc = _mm('bqhe,bkhe->bhqk', q, k) * HEAD ** -0.5
    causal = jnp.arange(s)[:, None] >= jnp.arange(s)[None, :]
    p = jax.nn.softmax(jnp.where(causal, sc, -1e30), axis=-1).astype(jnp.bfloat16)
    o = _mm('bhqk,bkhe->bqhe', p, v).astype(jnp.bfloat16).reshape(b, s, nh * HEAD)
    a = (h0.astype(jnp.float32) + _mm('bse,ed->bsd', o, wo)).astype(jnp.bfloat16)
    x2 = _rms(a, ln_ffn)
    hs = (jax.nn.silu(_mm('bsd,df->bsf', x2, ws1)) * _mm('bsd,df->bsf', x2, ws3)).astype(jnp.bfloat16)
    return a, _mm('bsf,fd->bsd', hs, ws2)


def _gate(u, wr, gi):
    lg = _mm('td,de->te', u, wr)
    hit = gi[..., None] == jnp.arange(wr.shape[1], dtype=gi.dtype)
    return jax.nn.softmax(jnp.sum(jnp.where(hit, lg[:, None, :], 0.0), axis=-1), axis=-1)


def _parts(c):
    hi = c.astype(jnp.bfloat16)
    r = c - hi.astype(jnp.float32)
    mid = r.astype(jnp.bfloat16)
    lo = (r - mid.astype(jnp.float32)).astype(jnp.bfloat16)
    return hi, mid, lo


CYCLE = [(0, 0), (1, 0), (2, 0), (3, 0), (3, 1), (2, 1), (1, 1), (0, 1)]


def _perms():
    n = len(CYCLE)
    dev = [[(z * 2 + y) * 2 + c for c in range(2)] for z, y in CYCLE]
    ahead = [(dev[p][0], dev[(p + 1) % n][0]) for p in range(n)]
    ahead += [(dev[p][1], dev[(p - 1) % n][1]) for p in range(n)]
    behind = [(b, a) for a, b in ahead]
    swap = [(dev[p][c], dev[p][1 - c]) for p in range(n) for c in range(2)]
    return ahead, behind, swap


def solution(mesh):
    g_ = mesh.shape['ep']
    assert g_ == 2 * len(CYCLE)
    rows = P(('dp', 'ep'))
    rep = P()
    ahead, behind, swap_p = _perms()

    def fwd(x):
        return jax.tree.map(lambda t: lax.ppermute(t, 'ep', ahead), x)

    def bwd(x):
        return jax.tree.map(lambda t: lax.ppermute(t, 'ep', behind), x)

    def swap(x):
        return jax.tree.map(lambda t: lax.ppermute(t, 'ep', swap_p), x)

    def local(h0, idx, slot, ln_attn, wq, wk, wv, wo, ln_ffn, ws1, ws3, ws2, ln_moe, wr, ue1, ue3, ue2):
        b, s, d = h0.shape
        top = idx.shape[-1]
        el = ue1.shape[0]
        ne = el * g_
        t = b * s
        cap = CAP_FACTOR * t * top // ne
        nr = el * cap
        u = _rms(h0, ln_moe).reshape(t, d)
        gi = idx.reshape(t, top)
        gate = _gate(u, wr, gi)
        pos = gi * cap + slot.reshape(t, top)
        meta = jnp.concatenate([pos.astype(jnp.float32).T, gate.T], axis=0)
        base = lax.axis_index('ep') * nr
        rowid = (base + jnp.arange(nr, dtype=jnp.int32)).astype(jnp.float32)

        def experts(pair):
            us = jnp.stack([x for x, _ in pair])
            ms = jnp.stack([m for _, m in pair])
            hit = ms[:, :top, None, :] == rowid[None, None, :, None]
            disp = jnp.any(hit, axis=1).astype(jnp.bfloat16)
            x = _mm('grt,gtd->grd', disp, us).astype(jnp.bfloat16)
            x = x.reshape(len(pair), el, cap, d)
            he = (jax.nn.silu(_mm('gecd,edf->gecf', x, ue1)) * _mm('gecd,edf->gecf', x, ue3)).astype(jnp.bfloat16)
            y = _mm('gecf,efd->gecd', he, ue2).astype(jnp.bfloat16).reshape(len(pair), nr, d)
            comb = jnp.sum(jnp.where(hit, ms[:, top:, None, :], 0.0), axis=1)
            m = sum(_mm('grt,grd->gtd', p, y) for p in _parts(comb))
            return [m[i] for i in range(len(pair))]

        own = (u, meta)
        own_o = swap(own)
        near, far = [], []
        a_, b_ = own, own
        half = t // 2
        for _ in range(3):
            a_, b_ = fwd(a_), bwd(b_)
            near.append(a_)
            far.append(b_)
        first = fwd((a_[0][:half], a_[1][:, :half]))
        last = bwd((b_[0][half:], b_[1][:, half:]))
        opp = (jnp.concatenate([first[0], last[0]], 0), jnp.concatenate([first[1], last[1]], 1))
        same = near + [opp] + far[::-1]
        other = [swap(x) for x in same]
        run = None
        for st in range(7):
            mine, theirs = experts([same[st], other[st]])
            q = mine + swap(theirs)
            run = fwd(q if run is None else run + q)
        mine, theirs = experts([own, own_o])
        a, fo = _dense(h0, ln_attn, wq, wk, wv, wo, ln_ffn, ws1, ws3, ws2)
        m = mine + swap(theirs) + run
        out = a.astype(jnp.float32) + fo + m.reshape(b, s, d)
        return out.astype(jnp.bfloat16)

    specs = (rows, rows, rows) + (rep,) * 11 + (P('ep'), P('ep'), P('ep'))
    return jax.shard_map(local, mesh=mesh, in_specs=specs, out_specs=rows, check_vma=False)
```

```python
import functools

import jax
import jax.numpy as jnp
from jax import lax
from jax.experimental import pallas as pl
from jax.experimental.pallas import tpu as pltpu
from jax.sharding import PartitionSpec as P


NRING = 2
F32, BF = jnp.float32, jnp.bfloat16
HEAD, EPS, QB = 128, 1e-6, 256
def _dot(a, b): return jnp.dot(a, b, preferred_element_type=F32)
def _dot_t(a, b): return lax.dot_general(a, b, (((1,), (1,)), ((), ())), preferred_element_type=F32)
ANY = pl.BlockSpec(memory_space=pl.ANY)

def _norm(x, w):
    xf = x.astype(F32)
    r = lax.rsqrt(jnp.mean(xf * xf, axis=-1, keepdims=True) + EPS)
    return (xf * r * w.astype(F32)).astype(BF)

def _attn_kernel(h_ref, ln_ref, cs_ref, sn_ref, wq_ref, wk_ref, wv_ref, *rest):
    o_ref, x1, qs, ks, vs = rest[-5:]
    s = h_ref.shape[0]
    @pl.when(pl.program_id(0) == 0)
    def _():
        @pl.loop(0, s // 128)
        def _(i):
            q = pl.ds(pl.multiple_of(i * 128, 128), 128)
            x1[q, :] = _norm(h_ref[q, :], ln_ref[...])
    for w, dst, rot in ((wq_ref, qs, True), (wk_ref, ks, True), (wv_ref, vs, False)):
        y = _dot(x1[...], w[...])
        if rot:
            for h in range(w.shape[1] // HEAD):
                c = slice(h * HEAD, (h + 1) * HEAD)
                x = y[:, c]
                dst[:, c] = (x * cs_ref[...] + pltpu.roll(x, HEAD // 2, 1) * sn_ref[...]).astype(BF)
        else:
            dst[...] = y.astype(BF)
    for h in range(qs.shape[1] // HEAD):
        c = slice(h * HEAD, (h + 1) * HEAD)
        for i in range(s // QB):
            n = (i + 1) * QB
            sc = _dot_t(qs[i * QB:n, c], ks[0:n, c])
            d = sc[:, i * QB:]
            low = lax.broadcasted_iota(jnp.int32, (QB, QB), 0) >= lax.broadcasted_iota(jnp.int32, (QB, QB), 1)
            d = jnp.where(low, d, -1e30)
            sc = jnp.concatenate([sc[:, :i * QB], d], axis=1) if i else d
            m = jnp.max(sc, axis=-1, keepdims=True)
            p = jnp.exp((sc - m) * HEAD ** -0.5)
            p = (p * (1.0 / jnp.sum(p, axis=-1, keepdims=True))).astype(BF)
            o_ref[i * QB:n, c] = _dot(p, vs[0:n, c]).astype(BF)

def _attn(h, ln, cs, sn, wq, wk, wv, deps=()):
    s, d = h.shape
    e = wq.shape[1]
    nb = 256
    whole = lambda a: pl.BlockSpec(a.shape, lambda i: (0,) * a.ndim)
    col = pl.BlockSpec((d, nb), lambda i: (0, i))
    return pl.pallas_call(
        _attn_kernel, grid=(e // nb,),
        out_shape=jax.ShapeDtypeStruct((s, e), BF),
        in_specs=[whole(h), whole(ln), whole(cs), whole(sn), col, col, col] + [ANY] * len(deps),
        out_specs=pl.BlockSpec((s, nb), lambda i: (0, i)),
        scratch_shapes=[pltpu.VMEM((s, d), BF)] + [pltpu.VMEM((s, nb), BF)] * 3,
        compiler_params=pltpu.CompilerParams(vmem_limit_bytes=64000000, dimension_semantics=("arbitrary",)),
        cost_estimate=pl.CostEstimate(flops=6 * s * d * e + 4 * s * s * e, bytes_accessed=6 * d * e + 4 * s * d, transcendentals=0),
        name="attention",
    )(h, ln, cs, sn, wq, wk, wv, *deps)

def _ffn_kernel(n1, n2, h_ref, o_ref, ln_ref, wo_ref, w1_ref, w3_ref, w2_ref, *rest):
    out_ref, a, x2, sb = rest[-4:]
    i = pl.program_id(0)
    nb = wo_ref.shape[1]
    fb = w1_ref.shape[1]
    @pl.when(i < n1)
    def _():
        c = pl.ds(pl.multiple_of(i * nb, nb), nb)
        a[:, c] = (h_ref[:, c].astype(F32) + _dot(o_ref[...], wo_ref[...])).astype(BF)
    @pl.when(i == n1)
    def _():
        @pl.loop(0, a.shape[0] // 128)
        def _(j):
            q = pl.ds(pl.multiple_of(j * 128, 128), 128)
            x2[q, :] = _norm(a[q, :], ln_ref[...])
    @pl.when((i >= n1) & (i < n1 + n2))
    def _():
        g = _dot(x2[...], w1_ref[...])
        v = _dot(x2[...], w3_ref[...])
        sb[:, pl.ds(pl.multiple_of((i - n1) * fb, fb), fb)] = (g * jax.nn.sigmoid(g) * v).astype(BF)
    @pl.when(i >= n1 + n2)
    def _():
        c = pl.ds(pl.multiple_of((i - n1 - n2) * nb, nb), nb)
        out_ref[...] = a[:, c].astype(F32) + _dot(sb[...], w2_ref[...])

def _ffn(h, o, ln, wo, w1, w3, w2, deps=()):
    s, d = h.shape
    f = w1.shape[1]
    nb, fb = 512, 256
    n1, n2, n3 = d // nb, f // fb, d // nb
    whole = lambda a: pl.BlockSpec(a.shape, lambda i: (0,) * a.ndim)
    return pl.pallas_call(
        functools.partial(_ffn_kernel, n1, n2), grid=(n1 + n2 + n3,),
        out_shape=jax.ShapeDtypeStruct((s, d), F32),
        in_specs=[whole(h), whole(o), whole(ln),
                  pl.BlockSpec((d, nb), lambda i: (0, jnp.minimum(i, n1 - 1))),
                  pl.BlockSpec((d, fb), lambda i: (0, jnp.clip(i - n1, 0, n2 - 1))),
                  pl.BlockSpec((d, fb), lambda i: (0, jnp.clip(i - n1, 0, n2 - 1))),
                  pl.BlockSpec((f, nb), lambda i: (0, jnp.clip(i - n1 - n2, 0, n3 - 1)))] + [ANY] * len(deps),
        out_specs=pl.BlockSpec((s, nb), lambda i: (0, jnp.clip(i - n1 - n2, 0, n3 - 1))),
        scratch_shapes=[pltpu.VMEM((s, d), BF), pltpu.VMEM((s, d), BF), pltpu.VMEM((s, f), BF)],
        compiler_params=pltpu.CompilerParams(vmem_limit_bytes=64000000, dimension_semantics=("arbitrary",)),
        cost_estimate=pl.CostEstimate(flops=2 * s * d * d + 6 * s * d * f, bytes_accessed=2 * d * d + 6 * d * f + 12 * s * d, transcendentals=0),
        name="ffn",
    )(h, o, ln, wo, w1, w3, w2, *deps)

def _angles(s):
    half = HEAD // 2
    freq = 10000.0 ** (-jnp.arange(half, dtype=F32) / half)
    ang = jnp.arange(s, dtype=F32)[:, None] * freq[None, :]
    c, sn = jnp.cos(ang), jnp.sin(ang)
    return jnp.concatenate([c, c], axis=1), jnp.concatenate([-sn, sn], axis=1)


T, D, FE, EL, CAP, NR = 1024, 2048, 1408, 4, 192, 768
MB = 256

def _tables(meta, base, tab_ref):
    ix, sl, gt = meta[0:8], meta[8:16], meta[16:24]
    rows = [[], [], [], []]
    for e in range(EL):
        hit = ix == (base + e).astype(F32)
        s = jnp.sum(jnp.where(hit, sl + 1.0, 0.0), axis=0, keepdims=True) - 1.0
        g = jnp.sum(jnp.where(hit, gt, 0.0), axis=0, keepdims=True)
        hi = g.astype(BF).astype(F32)
        r = g - hi
        mid = r.astype(BF).astype(F32)
        lo = r - mid
        for lst, v in zip(rows, (s, hi, mid, lo)): lst.append(v)
    tab_ref[...] = jnp.concatenate(sum(rows, []), axis=0)

def _experts_kernel(nc, up_n, base_ref, m0_ref, m1_ref, u0, u1, w1, w3, w2, *rest):
    (p0, p1, ub, xy, b1, b3, b2, hb, cb, tab, tabt, stg, usem, wsem, osem) = rest[-15:]
    base = base_ref[0]
    def wcopies(e, slot):
        return [pltpu.make_async_copy(s.at[e], d.at[slot], wsem.at[i, slot]) for i, (s, d) in enumerate(((w1, b1), (w3, b3)))]
    def dcopy(e):
        return pltpu.make_async_copy(w2.at[e], b2, wsem.at[2, 0])
    ucs = [pltpu.make_async_copy(u, ub.at[i], usem.at[i]) for i, u in enumerate((u0, u1))]
    for c in ucs: c.start()
    for g, m in enumerate((m0_ref, m1_ref)):
        _tables(m[...], base, tab.at[g])
    for g in range(2):
        it = lax.broadcasted_iota(jnp.int32, (CAP, T), 0).astype(F32)
        for e in range(EL):
            hit = it == tab[g, e:e + 1, :]
            cb[e * CAP:(e + 1) * CAP, 0:T] = jnp.where(hit, 1.0, 0.0).astype(BF)
        ucs[g].wait()
        if g == 0:
            for c in wcopies(0, 0): c.start()
        else:
            dcopy(0).start()
            for c in wcopies(1, 1): c.start()
        @pl.loop(0, D // nc)
        def _(n):
            c = pl.ds(pl.multiple_of(n * nc, nc), nc)
            x = _dot(cb[0:NR, 0:T], ub[g, :, c]).astype(BF)
            for e in range(EL):
                xy[pl.ds(e * 2 * CAP + g * CAP, CAP), c] = x[e * CAP:(e + 1) * CAP]
    @pl.loop(0, EL)
    def _(e):
        slot = lax.rem(e, 2)
        cs = wcopies(e, slot)
        cs[0].wait(); cs[1].wait()
        r = pl.ds(pl.multiple_of(e * 2 * CAP, 2 * CAP), 2 * CAP)
        if up_n == 0:
            g_ = _dot(xy[r, :], b1[slot]); v_ = _dot(xy[r, :], b3[slot])
            hb[...] = (g_ * jax.nn.sigmoid(g_) * v_).astype(BF)
        else:
            for n0 in range(0, FE // 256 * 256, up_n):
                k = min(up_n, FE // 256 * 256 - n0)
                g_ = _dot(xy[r, :], b1[slot, :, n0:n0 + k]); v_ = _dot(xy[r, :], b3[slot, :, n0:n0 + k])
                hb[:, n0:n0 + k] = (g_ * jax.nn.sigmoid(g_) * v_).astype(BF)
            n0 = FE // 256 * 256
            w = jnp.concatenate([b1[slot, :, n0:], b3[slot, :, n0:]], axis=1)
            gv = _dot(xy[r, :], w)
            g_, v_ = gv[:, :FE - n0], gv[:, FE - n0:]
            hb[:, n0:] = (g_ * jax.nn.sigmoid(g_) * v_).astype(BF)
        @pl.when(e + 2 < EL)
        def _():
            for c in wcopies(e + 2, slot): c.start()
        dcopy(e).wait()
        @pl.loop(0, D // nc)
        def _(n):
            c = pl.ds(pl.multiple_of(n * nc, nc), nc)
            xy[r, c] = _dot(hb[...], b2[:, c]).astype(BF)
        @pl.when(e + 1 < EL)
        def _():
            dcopy(e + 1).start()
    steps = D // nc
    for g, p in enumerate((p0, p1)):
        tabt[...] = jnp.concatenate([tab[g], jnp.zeros((112, T), F32)], axis=0).T
        @pl.loop(0, T // 128)
        def _(i):
            q = pl.ds(pl.multiple_of(i * 128, 128), 128)
            tt = tabt[q, :]
            for e2 in range(2):
                k = (lax.broadcasted_iota(jnp.int32, (128, 2 * CAP), 1)).astype(F32)
                ea, eb = 2 * e2, 2 * e2 + 1
                ha = k == tt[:, ea:ea + 1]
                hb_ = k == jnp.where(tt[:, eb:eb + 1] >= 0.0, tt[:, eb:eb + 1] + float(CAP), -1.0)
                for part in range(3):
                    o = 4 * (part + 1)
                    cc = jnp.where(ha, tt[:, o + ea:o + ea + 1], jnp.where(hb_, tt[:, o + eb:o + eb + 1], 0.0))
                    cb[q, part * NR + e2 * 2 * CAP: part * NR + (e2 + 1) * 2 * CAP] = cc.astype(BF)
        def oc(n): return pltpu.make_async_copy(stg.at[lax.rem(n, 2)], p.at[:, pl.ds(pl.multiple_of(n * nc, nc), nc)], osem.at[lax.rem(n, 2)])
        @pl.loop(0, steps)
        def _(n):
            c = pl.ds(pl.multiple_of(n * nc, nc), nc)
            y = jnp.concatenate([xy[e * 2 * CAP + g * CAP:e * 2 * CAP + (g + 1) * CAP, c] for e in range(EL)], axis=0)
            @pl.when(n >= 2)
            def _(): oc(n - 2).wait()
            y3 = jnp.concatenate([y, y, y], axis=0)
            for mb in range(0, T, MB):
                acc = _dot(cb[mb:mb + MB, :], y3)
                stg[lax.rem(n, 2), mb:mb + MB] = acc
            oc(n).start()
        oc(steps - 2).wait(); oc(steps - 1).wait()

def _experts(base, m0, m1, u0, u1, w1, w3, w2, deps=(), nc=512, up_n=256):
    anys = pl.BlockSpec(memory_space=pl.ANY)
    vm = pl.BlockSpec(memory_space=pltpu.VMEM)
    fl = 2 * 2 * (NR * T * D + NR * D * FE * 3 + 3 * T * NR * D)
    return pl.pallas_call(
        functools.partial(_experts_kernel, nc, up_n),
        out_shape=[jax.ShapeDtypeStruct((T, D), F32)] * 2,
        in_specs=[pl.BlockSpec(memory_space=pltpu.SMEM), vm, vm] + [anys] * (5 + len(deps)),
        out_specs=[anys] * 2,
        scratch_shapes=[
            pltpu.VMEM((2, T, D), BF), pltpu.VMEM((2 * NR, D), BF),
            pltpu.VMEM((2, D, FE), BF), pltpu.VMEM((2, D, FE), BF), pltpu.VMEM((FE, D), BF),
            pltpu.VMEM((2 * CAP, FE), BF), pltpu.VMEM((T, 3 * NR), BF),
            pltpu.VMEM((2, 16, T), F32), pltpu.VMEM((T, 128), F32),
            pltpu.VMEM((2, T, nc), F32),
            pltpu.SemaphoreType.DMA((2,)), pltpu.SemaphoreType.DMA((3, 2)), pltpu.SemaphoreType.DMA((2,)),
        ],
        compiler_params=pltpu.CompilerParams(vmem_limit_bytes=67043328),
        cost_estimate=pl.CostEstimate(flops=fl, bytes_accessed=120_000_000, transcendentals=0),
        name="experts",
    )(base, m0, m1, u0, u1, w1, w3, w2, *deps)


def _sum_kernel(n, *refs):
    acc = refs[0][...]
    for r in refs[1:n]:
        acc = acc + r[...]
    refs[-1][...] = acc.astype(refs[-1].dtype)


def _sum(parts, dtype, width, deps=(), into=None):
    s = parts[0][0].shape[0]
    rb = 256
    spec = lambda c: pl.BlockSpec((rb, width), lambda i, c=c: (i, c))
    extra = list(deps) + ([into[0]] if into and into[0] is not None else [])
    alias = {len(parts) + len(deps): 0} if into and into[0] is not None else {}
    return pl.pallas_call(
        functools.partial(_sum_kernel, len(parts)), grid=(s // rb,),
        out_shape=jax.ShapeDtypeStruct((s, into[2] if into else width), dtype),
        in_specs=[spec(c) for _, c in parts] + [ANY] * len(extra),
        out_specs=spec(into[1] if into else 0),
        input_output_aliases=alias,
        compiler_params=pltpu.CompilerParams(dimension_semantics=("arbitrary",)),
        cost_estimate=pl.CostEstimate(flops=3 * s * width * 1000, bytes_accessed=16 * s * width, transcendentals=0),
        name="ring_sum",
    )(*[a for a, _ in parts], *extra)

def _gate(u, wr, gi):
    lg = jnp.einsum('td,de->te', u, wr, preferred_element_type=F32)
    hit = gi[..., None] == jnp.arange(wr.shape[1], dtype=gi.dtype)
    return jax.nn.softmax(jnp.sum(jnp.where(hit, lg[:, None, :], 0.0), axis=-1), axis=-1)


CYCLE = [(0, 0), (1, 0), (2, 0), (3, 0), (3, 1), (2, 1), (1, 1), (0, 1)]


def _perms():
    n = len(CYCLE)
    dev = [[(z * 2 + y) * 2 + c for c in range(2)] for z, y in CYCLE]
    ahead = [(dev[p][0], dev[(p + 1) % n][0]) for p in range(n)]
    ahead += [(dev[p][1], dev[(p - 1) % n][1]) for p in range(n)]
    behind = [(b, a) for a, b in ahead]
    swap = [(dev[p][c], dev[p][1 - c]) for p in range(n) for c in range(2)]
    return ahead, behind, swap


def solution(mesh):
    g_ = mesh.shape['ep']
    assert g_ == 2 * len(CYCLE)
    rows = P(('dp', 'ep'))
    rep = P()
    ahead, behind, swap_p = _perms()

    def send(x, perm):
        return jax.tree.map(lambda t: lax.ppermute(t, 'ep', perm), x)

    def local(h0, idx, slot, ln_attn, wq, wk, wv, wo, ln_ffn, ws1, ws3, ws2, ln_moe, wr, ue1, ue3, ue2):
        b, s, d = h0.shape
        top = idx.shape[-1]
        el = ue1.shape[0]
        assert (b, s, d) == (1, T, D) and ue1.shape == (EL, D, FE) and top <= 8
        h = h0.reshape(s, d)
        u = _norm(h, ln_moe)
        gi = idx.reshape(s, top)
        gate = _gate(u, wr, gi)

        def pad(x, v):
            return jnp.pad(x.astype(F32).T, ((0, 8 - top), (0, 0)), constant_values=v)

        meta = jnp.concatenate([pad(gi, -1.0), pad(slot.reshape(s, top), 0.0), pad(gate, 0.0)], axis=0)
        base = (lax.axis_index('ep') * el).astype(jnp.int32).reshape(1)
        width = d // NRING
        run = [None] * NRING

        def experts(x, y, *deps):
            mine, theirs = _experts(base, x[1], y[1], x[0], y[0], ue1, ue3, ue2, deps)
            return mine, send(theirs, swap_p)

        def ring(pair, *deps):
            for i in range(NRING):
                parts = ([(run[i], 0)] if run[i] is not None else []) + [(pair[0], i), (pair[1], i)]
                part = _sum(parts, F32, width, deps)
                run[i], deps = send(part, ahead), (part,)
            return part

        own = (u, meta)
        own_o = send(own, swap_p)
        f0, b0 = send(own, ahead), send(own, behind)
        o = _attn(h, ln_attn[None], *_angles(s), wq, wk, wv, (u,))
        f0, b0, o = lax.optimization_barrier((f0, b0, o))
        f1, b1 = send(f0, ahead), send(b0, behind)
        p0 = experts(f0, send(f0, swap_p), o)
        f1, b1, m0 = lax.optimization_barrier((f1, b1, p0[0]))
        f2, b2 = send(f1, ahead), send(b1, behind)
        r = ring((m0, p0[1]), f1[0], b1[0])
        af = _ffn(h, o, ln_ffn[None], wo, ws1, ws3, ws2, (r,))
        p1 = experts(f1, send(f1, swap_p), af)
        f2, b2, m1 = lax.optimization_barrier((f2, b2, p1[0]))
        f3 = send(f2, ahead)
        pair = experts(f2, send(f2, swap_p), m1)
        r = ring((m1, p1[1]), pair[0])
        for x in (f3, b2, b1, b0, own):
            y = own_o if x is own else send(x, swap_p)
            nxt = experts(x, y, r)
            r = ring(pair, nxt[0])
            pair = nxt
        out = None
        for i in range(NRING):
            out = _sum([(af, i), (pair[0], i), (pair[1], i), (run[i], 0)], jnp.bfloat16, width, (), (out, i, d))
        return out.reshape(b, s, d)

    specs = (rows, rows, rows) + (rep,) * 11 + (P('ep'), P('ep'), P('ep'))
    return jax.shard_map(local, mesh=mesh, in_specs=specs, out_specs=rows, check_vma=False)
```

```python
import functools

import jax
import jax.numpy as jnp
import numpy as np
from jax import lax
from jax.experimental import pallas as pl
from jax.experimental.pallas import tpu as pltpu
from jax.sharding import PartitionSpec as P


NRING = 2
F32, BF = jnp.float32, jnp.bfloat16
HEAD, EPS, QB = 128, 1e-6, 256
def _dot(a, b): return jnp.dot(a, b, preferred_element_type=F32)
def _dot_t(a, b): return lax.dot_general(a, b, (((1,), (1,)), ((), ())), preferred_element_type=F32)
ANY = pl.BlockSpec(memory_space=pl.ANY)

def _norm(x, w):
    xf = x.astype(F32)
    r = lax.rsqrt(jnp.mean(xf * xf, axis=-1, keepdims=True) + EPS)
    return (xf * r * w.astype(F32)).astype(BF)

def _attn_kernel(h_ref, ln_ref, cs_ref, sn_ref, wq_ref, wk_ref, wv_ref, *rest):
    o_ref, x1, qs, ks, vs = rest[-5:]
    s = h_ref.shape[0]
    @pl.when(pl.program_id(0) == 0)
    def _():
        @pl.loop(0, s // 128)
        def _(i):
            q = pl.ds(pl.multiple_of(i * 128, 128), 128)
            x1[q, :] = _norm(h_ref[q, :], ln_ref[...])
    for w, dst, rot in ((wq_ref, qs, True), (wk_ref, ks, True), (wv_ref, vs, False)):
        y = _dot(x1[...], w[...])
        if rot:
            for h in range(w.shape[1] // HEAD):
                c = slice(h * HEAD, (h + 1) * HEAD)
                x = y[:, c]
                dst[:, c] = (x * cs_ref[...] + pltpu.roll(x, HEAD // 2, 1) * sn_ref[...]).astype(BF)
        else:
            dst[...] = y.astype(BF)
    for h in range(qs.shape[1] // HEAD):
        c = slice(h * HEAD, (h + 1) * HEAD)
        for i in range(s // QB):
            n = (i + 1) * QB
            sc = _dot_t(qs[i * QB:n, c], ks[0:n, c])
            d = sc[:, i * QB:]
            low = lax.broadcasted_iota(jnp.int32, (QB, QB), 0) >= lax.broadcasted_iota(jnp.int32, (QB, QB), 1)
            d = jnp.where(low, d, -1e30)
            sc = jnp.concatenate([sc[:, :i * QB], d], axis=1) if i else d
            m = jnp.max(sc, axis=-1, keepdims=True)
            p = jnp.exp((sc - m) * HEAD ** -0.5)
            p = (p * (1.0 / jnp.sum(p, axis=-1, keepdims=True))).astype(BF)
            o_ref[i * QB:n, c] = _dot(p, vs[0:n, c]).astype(BF)

def _attn(h, ln, cs, sn, wq, wk, wv, deps=()):
    s, d = h.shape
    e = wq.shape[1]
    nb = 256
    whole = lambda a: pl.BlockSpec(a.shape, lambda i: (0,) * a.ndim)
    col = pl.BlockSpec((d, nb), lambda i: (0, i))
    return pl.pallas_call(
        _attn_kernel, grid=(e // nb,),
        out_shape=jax.ShapeDtypeStruct((s, e), BF),
        in_specs=[whole(h), whole(ln), whole(cs), whole(sn), col, col, col] + [ANY] * len(deps),
        out_specs=pl.BlockSpec((s, nb), lambda i: (0, i)),
        scratch_shapes=[pltpu.VMEM((s, d), BF)] + [pltpu.VMEM((s, nb), BF)] * 3,
        compiler_params=pltpu.CompilerParams(vmem_limit_bytes=64000000, dimension_semantics=("arbitrary",)),
        cost_estimate=pl.CostEstimate(flops=6 * s * d * e + 4 * s * s * e, bytes_accessed=6 * d * e + 4 * s * d, transcendentals=0),
        name="attention",
    )(h, ln, cs, sn, wq, wk, wv, *deps)

def _ffn_kernel(n1, n2, h_ref, o_ref, ln_ref, wo_ref, w1_ref, w3_ref, w2_ref, *rest):
    out_ref, a, x2, sb = rest[-4:]
    i = pl.program_id(0)
    nb = wo_ref.shape[1]
    fb = w1_ref.shape[1]
    @pl.when(i < n1)
    def _():
        c = pl.ds(pl.multiple_of(i * nb, nb), nb)
        a[:, c] = (h_ref[:, c].astype(F32) + _dot(o_ref[...], wo_ref[...])).astype(BF)
    @pl.when(i == n1)
    def _():
        @pl.loop(0, a.shape[0] // 128)
        def _(j):
            q = pl.ds(pl.multiple_of(j * 128, 128), 128)
            x2[q, :] = _norm(a[q, :], ln_ref[...])
    @pl.when((i >= n1) & (i < n1 + n2))
    def _():
        g = _dot(x2[...], w1_ref[...])
        v = _dot(x2[...], w3_ref[...])
        sb[:, pl.ds(pl.multiple_of((i - n1) * fb, fb), fb)] = (g * jax.nn.sigmoid(g) * v).astype(BF)
    @pl.when(i >= n1 + n2)
    def _():
        c = pl.ds(pl.multiple_of((i - n1 - n2) * nb, nb), nb)
        out_ref[...] = a[:, c].astype(F32) + _dot(sb[...], w2_ref[...])

def _ffn(h, o, ln, wo, w1, w3, w2, deps=()):
    s, d = h.shape
    f = w1.shape[1]
    nb, fb = 512, 256
    n1, n2, n3 = d // nb, f // fb, d // nb
    whole = lambda a: pl.BlockSpec(a.shape, lambda i: (0,) * a.ndim)
    return pl.pallas_call(
        functools.partial(_ffn_kernel, n1, n2), grid=(n1 + n2 + n3,),
        out_shape=jax.ShapeDtypeStruct((s, d), F32),
        in_specs=[whole(h), whole(o), whole(ln),
                  pl.BlockSpec((d, nb), lambda i: (0, jnp.minimum(i, n1 - 1))),
                  pl.BlockSpec((d, fb), lambda i: (0, jnp.clip(i - n1, 0, n2 - 1))),
                  pl.BlockSpec((d, fb), lambda i: (0, jnp.clip(i - n1, 0, n2 - 1))),
                  pl.BlockSpec((f, nb), lambda i: (0, jnp.clip(i - n1 - n2, 0, n3 - 1)))] + [ANY] * len(deps),
        out_specs=pl.BlockSpec((s, nb), lambda i: (0, jnp.clip(i - n1 - n2, 0, n3 - 1))),
        scratch_shapes=[pltpu.VMEM((s, d), BF), pltpu.VMEM((s, d), BF), pltpu.VMEM((s, f), BF)],
        compiler_params=pltpu.CompilerParams(vmem_limit_bytes=64000000, dimension_semantics=("arbitrary",)),
        cost_estimate=pl.CostEstimate(flops=2 * s * d * d + 6 * s * d * f, bytes_accessed=2 * d * d + 6 * d * f + 12 * s * d, transcendentals=0),
        name="ffn",
    )(h, o, ln, wo, w1, w3, w2, *deps)

def _angles(s):
    half = HEAD // 2
    freq = 10000.0 ** (-jnp.arange(half, dtype=F32) / half)
    ang = jnp.arange(s, dtype=F32)[:, None] * freq[None, :]
    c, sn = jnp.cos(ang), jnp.sin(ang)
    return jnp.concatenate([c, c], axis=1), jnp.concatenate([-sn, sn], axis=1)


T, D, FE, EL, CAP, NR = 1024, 2048, 1408, 4, 192, 768
MB = 1024

def _tables(meta, base, tab_ref):
    ix, sl, gt = meta[0:8], meta[8:16], meta[16:24]
    rows = [[], [], [], []]
    for e in range(EL):
        hit = ix == (base + e).astype(F32)
        s = jnp.sum(jnp.where(hit, sl + 1.0, 0.0), axis=0, keepdims=True) - 1.0
        g = jnp.sum(jnp.where(hit, gt, 0.0), axis=0, keepdims=True)
        hi = g.astype(BF).astype(F32)
        r = g - hi
        mid = r.astype(BF).astype(F32)
        lo = r - mid
        for lst, v in zip(rows, (s, hi, mid, lo)): lst.append(v)
    tab_ref[...] = jnp.concatenate(sum(rows, []), axis=0)

def _select_block(tt, cb, q, o0):
    n = tt.shape[0]
    for e2 in range(2):
        k = (lax.broadcasted_iota(jnp.int32, (n, 2 * CAP), 1)).astype(F32)
        ea, eb = 2 * e2, 2 * e2 + 1
        ha = k == tt[:, ea:ea + 1]
        hb = k == jnp.where(tt[:, eb:eb + 1] >= 0.0, tt[:, eb:eb + 1] + float(CAP), -1.0)
        for part in range(3):
            o = 4 * (part + 1)
            cc = jnp.where(ha, tt[:, o + ea:o + ea + 1], jnp.where(hb, tt[:, o + eb:o + eb + 1], 0.0))
            c0 = o0 + part * NR + e2 * 2 * CAP
            cb[q, c0:c0 + 2 * CAP] = cc.astype(BF)

def _columns(tab):
    return jnp.concatenate([tab, jnp.zeros((112, T), F32)], axis=0).T

def _experts_kernel(nc, up_n, raw, base_ref, m0_ref, m1_ref, u0, u1, w1, w3, w2, *rest):
    ub, xy, b1, b3, b2, hb, cb, tab, tabt, stg, usem, wsem, osem = rest[-13:]
    outs = rest[-15:-13] if raw else rest[-16:-13]
    base = base_ref[0]
    def wcopies(e, slot):
        return [pltpu.make_async_copy(s.at[e], d.at[slot], wsem.at[i, slot]) for i, (s, d) in enumerate(((w1, b1), (w3, b3)))]
    def dcopy(e):
        return pltpu.make_async_copy(w2.at[e], b2, wsem.at[2, 0])
    def ycopies(e):
        return [pltpu.make_async_copy(xy.at[pl.ds(pl.multiple_of((2 * e + g) * CAP, CAP), CAP)], p.at[pl.ds(pl.multiple_of(e * CAP, CAP), CAP)], osem.at[g]) for g, p in enumerate(outs)]
    ucs = [pltpu.make_async_copy(u, ub.at[i], usem.at[i]) for i, u in enumerate((u0, u1))]
    for c in ucs: c.start()
    for g, m in enumerate((m0_ref, m1_ref)):
        _tables(m[...], base, tab.at[g])
    for g in range(2):
        it = lax.broadcasted_iota(jnp.int32, (CAP, T), 0).astype(F32)
        for e in range(EL):
            hit = it == tab[g, e:e + 1, :]
            cb[0, e * CAP:(e + 1) * CAP, g * T:(g + 1) * T] = jnp.where(hit, 1.0, 0.0).astype(BF)
        if not raw:
            tabt[g] = _columns(tab[g])
    for g in range(2):
        ucs[g].wait()
        if g == 0:
            for c in wcopies(0, 0): c.start()
        else:
            dcopy(0).start()
            for c in wcopies(1, 1): c.start()
        @pl.loop(0, D // nc)
        def _(n):
            c = pl.ds(pl.multiple_of(n * nc, nc), nc)
            x = _dot(cb[0, 0:NR, g * T:(g + 1) * T], ub[g, :, c]).astype(BF)
            for e in range(EL):
                xy[pl.ds(e * 2 * CAP + g * CAP, CAP), c] = x[e * CAP:(e + 1) * CAP]
    @pl.loop(0, EL)
    def _(e):
        slot = lax.rem(e, 2)
        cs = wcopies(e, slot)
        cs[0].wait(); cs[1].wait()
        r = pl.ds(pl.multiple_of(e * 2 * CAP, 2 * CAP), 2 * CAP)
        if up_n == 0:
            g_ = _dot(xy[r, :], b1[slot]); v_ = _dot(xy[r, :], b3[slot])
            hb[...] = (g_ * jax.nn.sigmoid(g_) * v_).astype(BF)
        else:
            for n0 in range(0, FE // 256 * 256, up_n):
                k = min(up_n, FE // 256 * 256 - n0)
                g_ = _dot(xy[r, :], b1[slot, :, n0:n0 + k]); v_ = _dot(xy[r, :], b3[slot, :, n0:n0 + k])
                hb[:, n0:n0 + k] = (g_ * jax.nn.sigmoid(g_) * v_).astype(BF)
                if not raw and n0 // up_n < 4:
                    q = pl.ds(pl.multiple_of(lax.rem(e, 2) * 512 + n0 // up_n * 128, 128), 128)
                    _select_block(tabt[e // 2, q, :], cb.at[e // 2], q, 0)
            n0 = FE // 256 * 256
            w = jnp.concatenate([b1[slot, :, n0:], b3[slot, :, n0:]], axis=1)
            gv = _dot(xy[r, :], w)
            g_, v_ = gv[:, :FE - n0], gv[:, FE - n0:]
            hb[:, n0:] = (g_ * jax.nn.sigmoid(g_) * v_).astype(BF)
        @pl.when(e + 2 < EL)
        def _():
            for c in wcopies(e + 2, slot): c.start()
        dcopy(e).wait()
        @pl.loop(0, D // nc)
        def _(n):
            c = pl.ds(pl.multiple_of(n * nc, nc), nc)
            xy[r, c] = _dot(hb[...], b2[:, c]).astype(BF)
        @pl.when(e + 1 < EL)
        def _():
            dcopy(e + 1).start()
        if raw:
            for c in ycopies(e): c.start()
    if raw:
        @pl.loop(0, EL)
        def _(e):
            for c in ycopies(e): c.wait()
        return
    steps = D // nc
    def combine(g, p, first, steps):
        def oc(n): return pltpu.make_async_copy(stg.at[lax.rem(n, 2)], p.at[:, pl.ds(pl.multiple_of(n * nc, nc), nc)], osem.at[lax.rem(n, 2)])
        @pl.loop(0, steps)
        def _(n):
            c = pl.ds(pl.multiple_of((n + first) * nc, nc), nc)
            y = jnp.concatenate([xy[e * 2 * CAP + g * CAP:e * 2 * CAP + (g + 1) * CAP, c] for e in range(EL)], axis=0)
            @pl.when(n >= 2)
            def _(): oc(n - 2).wait()
            y3 = jnp.concatenate([y, y, y], axis=0)
            for mb in range(0, T, MB):
                stg[lax.rem(n, 2), mb:mb + MB] = _dot(cb[g, mb:mb + MB, :], y3)
            oc(n).start()
        oc(steps - 2).wait(); oc(steps - 1).wait()
    combine(0, outs[0], 0, steps)
    combine(1, outs[1], 0, steps // 2)
    combine(1, outs[2], steps // 2, steps // 2)

def _experts(base, m0, m1, u0, u1, w1, w3, w2, deps=(), raw=False, nc=512, up_n=256):
    shapes = [(NR, D)] * 2 if raw else [(T, D), (T, D // 2), (T, D // 2)]
    anys = pl.BlockSpec(memory_space=pl.ANY)
    vm = pl.BlockSpec(memory_space=pltpu.VMEM)
    fl = 2 * 2 * (NR * T * D + NR * D * FE * 3 + (0 if raw else 3 * T * NR * D))
    return pl.pallas_call(
        functools.partial(_experts_kernel, nc, up_n, raw),
        out_shape=[jax.ShapeDtypeStruct(x, BF if raw else F32) for x in shapes],
        in_specs=[pl.BlockSpec(memory_space=pltpu.SMEM), vm, vm] + [anys] * (5 + len(deps)),
        out_specs=[anys] * len(shapes),
        scratch_shapes=[
            pltpu.VMEM((2, T, D), BF), pltpu.VMEM((2 * NR, D), BF),
            pltpu.VMEM((2, D, FE), BF), pltpu.VMEM((2, D, FE), BF), pltpu.VMEM((FE, D), BF),
            pltpu.VMEM((2 * CAP, FE), BF), pltpu.VMEM((1 if raw else 2, T, 3 * NR), BF),
            pltpu.VMEM((2, 16, T), F32), pltpu.VMEM((2, T, 128), F32),
            pltpu.VMEM((2, T, nc), F32),
            pltpu.SemaphoreType.DMA((2,)), pltpu.SemaphoreType.DMA((3, 2)), pltpu.SemaphoreType.DMA((2,)),
        ],
        compiler_params=pltpu.CompilerParams(vmem_limit_bytes=67043328),
        cost_estimate=pl.CostEstimate(flops=fl, bytes_accessed=120_000_000, transcendentals=0),
        name="experts_rows" if raw else "experts",
    )(base, m0, m1, u0, u1, w1, w3, w2, *deps)

def _prep_kernel(base_ref, m_ref, *rest):
    out, tab, tabt = rest[-3:]
    _tables(m_ref[...], base_ref[pl.program_id(0)], tab)
    tabt[...] = _columns(tab[...])
    @pl.loop(0, T // 128)
    def _(i):
        q = pl.ds(pl.multiple_of(i * 128, 128), 128)
        _select_block(tabt[q, :], out, q, 0)

def _prep(bases, m, deps=()):
    return pl.pallas_call(
        _prep_kernel, grid=(2,),
        out_shape=jax.ShapeDtypeStruct((T, 6 * NR), BF),
        in_specs=[pl.BlockSpec(memory_space=pltpu.SMEM), pl.BlockSpec((24, T), lambda n: (0, 0))] + [pl.BlockSpec(memory_space=pl.ANY)] * len(deps),
        out_specs=pl.BlockSpec((T, 3 * NR), lambda n: (0, n)),
        scratch_shapes=[pltpu.VMEM((16, T), F32), pltpu.VMEM((T, 128), F32)],
        compiler_params=pltpu.CompilerParams(vmem_limit_bytes=64000000, dimension_semantics=("arbitrary",)),
        cost_estimate=pl.CostEstimate(flops=12 * T * NR * 200, bytes_accessed=12 * T * NR, transcendentals=0),
        name="gather_gates",
    )(bases, m, *deps)

def _gather_kernel(na, no, nc, cb, ya, yb, *rest):
    adds, halves, outs = rest[:na], rest[na:na + 2], rest[-no:]
    n = pl.program_id(0)
    y = jnp.concatenate([ya[...]] * 3 + [yb[...]] * 3, axis=0)
    per = D // nc // no
    for mb in range(0, T, MB):
        q = slice(mb, mb + MB)
        acc = _dot(cb[q, :], y)
        for a in adds: acc = acc + a[q, :]
        acc = acc + jnp.where(2 * n < D // nc, halves[0][q, :], halves[1][q, :])
        for j, o in enumerate(outs):
            if no == 1:
                o[q, :] = acc
            else:
                @pl.when(n // per == j)
                def _(o=o): o[q, :] = acc

def _gather(cb, ya, yb, adds, halves, no=1, deps=(), nc=512):
    anys = pl.BlockSpec(memory_space=pl.ANY)
    per = D // nc // no
    half = D // nc // 2
    blk = pl.BlockSpec((T, nc), lambda n: (0, n))
    row = pl.BlockSpec((NR, nc), lambda n: (0, n))
    return pl.pallas_call(
        functools.partial(_gather_kernel, len(adds), no, nc), grid=(D // nc,),
        out_shape=[jax.ShapeDtypeStruct((T, D // no), F32)] * no,
        in_specs=[pl.BlockSpec((T, 6 * NR), lambda n: (0, 0)), row, row] + [blk] * len(adds)
        + [pl.BlockSpec((T, nc), lambda n, j=j: (0, jnp.clip(n - j * half, 0, half - 1))) for j in range(2)] + [anys] * len(deps),
        out_specs=[pl.BlockSpec((T, nc), lambda n, j=j: (0, jnp.clip(n - j * per, 0, per - 1))) for j in range(no)],
        compiler_params=pltpu.CompilerParams(vmem_limit_bytes=64000000, dimension_semantics=("arbitrary",)),
        cost_estimate=pl.CostEstimate(flops=12 * T * NR * D, bytes_accessed=4 * NR * D + 4 * T * D * (1 + len(adds)), transcendentals=0),
        name="gather_rows",
    )(cb, ya, yb, *adds, *halves, *deps)


def _sum_kernel(n, *refs):
    acc = refs[0][...]
    for r in refs[1:n]:
        acc = acc + r[...]
    refs[-1][...] = acc.astype(refs[-1].dtype)


def _sum(parts, dtype, width, deps=(), into=None):
    s = parts[0][0].shape[0]
    rb = 256
    spec = lambda c: pl.BlockSpec((rb, width), lambda i, c=c: (i, c))
    extra = list(deps) + ([into[0]] if into and into[0] is not None else [])
    alias = {len(parts) + len(deps): 0} if into and into[0] is not None else {}
    return pl.pallas_call(
        functools.partial(_sum_kernel, len(parts)), grid=(s // rb,),
        out_shape=jax.ShapeDtypeStruct((s, into[2] if into else width), dtype),
        in_specs=[spec(c) for _, c in parts] + [ANY] * len(extra),
        out_specs=spec(into[1] if into else 0),
        input_output_aliases=alias,
        compiler_params=pltpu.CompilerParams(dimension_semantics=("arbitrary",)),
        cost_estimate=pl.CostEstimate(flops=3 * s * width * 1000, bytes_accessed=16 * s * width, transcendentals=0),
        name="ring_sum",
    )(*[a for a, _ in parts], *extra)

def _gate(u, wr, gi):
    lg = jnp.einsum('td,de->te', u, wr, preferred_element_type=F32)
    hit = gi[..., None] == jnp.arange(wr.shape[1], dtype=gi.dtype)
    return jax.nn.softmax(jnp.sum(jnp.where(hit, lg[:, None, :], 0.0), axis=-1), axis=-1)


CYCLE = [(0, 0), (1, 0), (2, 0), (3, 0), (3, 1), (2, 1), (1, 1), (0, 1)]
DEV = [[(z * 2 + y) * 2 + c for c in range(2)] for z, y in CYCLE]


def _perm(step, cross):
    n = len(CYCLE)
    sign = (-1, 1) if cross else (1, -1)
    return [(DEV[p][c], DEV[(p + sign[c] * step) % n][1 - c if cross else c]) for p in range(n) for c in range(2)]


def _from(step, el):
    n = len(CYCLE)
    t = np.zeros((2 * n, 2), np.int32)
    for p in range(n):
        for c in range(2):
            q = (p - (1, -1)[c] * step) % n
            t[DEV[p][c]] = (DEV[q][c] * el, DEV[q][1 - c] * el)
    return t


def solution(mesh):
    g_ = mesh.shape['ep']
    assert g_ == 2 * len(CYCLE)
    rows = P(('dp', 'ep'))
    rep = P()
    ahead, behind, swap_p = _perm(1, False), _perm(-1, False), _perm(0, True)

    def send(x, perm):
        return jax.tree.map(lambda t: lax.ppermute(t, 'ep', perm), x)

    def local(h0, idx, slot, ln_attn, wq, wk, wv, wo, ln_ffn, ws1, ws3, ws2, ln_moe, wr, ue1, ue3, ue2):
        b, s, d = h0.shape
        top = idx.shape[-1]
        el = ue1.shape[0]
        assert (b, s, d) == (1, T, D) and ue1.shape == (EL, D, FE) and top <= 8
        h = h0.reshape(s, d)
        u = _norm(h, ln_moe)
        gi = idx.reshape(s, top)
        gate = _gate(u, wr, gi)

        def pad(x, v):
            return jnp.pad(x.astype(F32).T, ((0, 8 - top), (0, 0)), constant_values=v)

        meta = jnp.concatenate([pad(gi, -1.0), pad(slot.reshape(s, top), 0.0), pad(gate, 0.0)], axis=0)
        me = lax.axis_index('ep')
        base = (me * el).astype(jnp.int32).reshape(1)
        base_up = jnp.asarray(_from(1, el))[me]
        base_down = jnp.asarray(_from(-1, el))[me]
        width = d // NRING

        def experts(x, y, *deps):
            mine, *theirs = _experts(base, x[1], y[1], x[0], y[0], ue1, ue3, ue2, deps)
            return mine, send(theirs, swap_p)

        def rows_of(x, y, *deps):
            return _experts(base, x[1], y[1], x[0], y[0], ue1, ue3, ue2, deps, raw=True)

        def ring(run, pair, *deps):
            out = []
            for i in range(NRING):
                part = _sum([(run[i], 0), (pair[0], i), (pair[1][i], 0)], F32, width, deps)
                deps = (part,)
                out.append(send(part, ahead))
            return out, part

        def gates(bases, m, *deps):
            return _prep(bases, m, deps)

        own = (u, meta)
        own_o = send(own, swap_p)
        f0, b0 = send(own, ahead), send(own, behind)
        o = _attn(h, ln_attn[None], *_angles(s), wq, wk, wv, (u,))
        f0, b0, o = lax.optimization_barrier((f0, b0, o))
        f1, b1 = send(f0, ahead), send(b0, behind)
        p6 = experts(b0, send(b0, swap_p), o)
        f1, b1, m6 = lax.optimization_barrier((f1, b1, p6[0]))
        p6 = m6, p6[1]
        f2, b2 = send(f1, ahead), send(b1, behind)
        r1 = rows_of(f1, send(f1, swap_p), m6)
        chain = send(r1[0], ahead), send(r1[1], _perm(1, True))
        r0 = rows_of(f0, send(f0, swap_p), r1[0])
        f2, b2, r00 = lax.optimization_barrier((f2, b2, r0[0]))
        direct = send(r00, behind), send(r0[1], _perm(-1, True))
        f3 = send(f2, ahead)
        p2 = experts(f2, send(f2, swap_p), r00)
        g2 = gates(base_up, f2[1], p2[0])
        af = _ffn(h, o, ln_ffn[None], wo, ws1, ws3, ws2, (g2,))
        q = _gather(g2, *chain, p2[:1], p2[1], NRING, (af,))
        run = [send(x, ahead) for x in q]
        g7 = gates(base_down, meta, q[0])
        p3 = experts(f3, send(f3, swap_p), g7)
        run, r = ring(run, p3)
        p4 = experts(b2, send(b2, swap_p), r)
        run, r = ring(run, p4)
        p5 = experts(b1, send(b1, swap_p), r)
        run, r = ring(run, p5)
        p7 = experts(own, own_o, r)
        run, r = ring(run, p6, p7[0])
        base_sum, = _gather(g7, *direct, (af, p7[0]), p7[1], 1, (r,))
        out = None
        for i in range(NRING):
            out = _sum([(base_sum, i), (run[i], 0)], jnp.bfloat16, width, (), (out, i, d))
        return out.reshape(b, s, d)

    specs = (rows, rows, rows) + (rep,) * 11 + (P('ep'), P('ep'), P('ep'))
    return jax.shard_map(local, mesh=mesh, in_specs=specs, out_specs=rows, check_vma=False)
```

```python
import functools

import jax
import jax.numpy as jnp
import numpy as np
from jax import lax
from jax.experimental import pallas as pl
from jax.experimental.pallas import tpu as pltpu
from jax.sharding import PartitionSpec as P


NRING = 2
F32, BF = jnp.float32, jnp.bfloat16
HEAD, EPS, QB = 128, 1e-6, 256
def _dot(a, b): return jnp.dot(a, b, preferred_element_type=F32)
def _dot_t(a, b): return lax.dot_general(a, b, (((1,), (1,)), ((), ())), preferred_element_type=F32)
ANY = pl.BlockSpec(memory_space=pl.ANY)

def _norm(x, w):
    xf = x.astype(F32)
    r = lax.rsqrt(jnp.mean(xf * xf, axis=-1, keepdims=True) + EPS)
    return (xf * r * w.astype(F32)).astype(BF)

def _attn_kernel(h_ref, ln_ref, cs_ref, sn_ref, wq_ref, wk_ref, wv_ref, *rest):
    o_ref, x1, qs, ks, vs = rest[-5:]
    s = h_ref.shape[0]
    @pl.when(pl.program_id(0) == 0)
    def _():
        @pl.loop(0, s // 128)
        def _(i):
            q = pl.ds(pl.multiple_of(i * 128, 128), 128)
            x1[q, :] = _norm(h_ref[q, :], ln_ref[...])
    for w, dst, rot in ((wq_ref, qs, True), (wk_ref, ks, True), (wv_ref, vs, False)):
        y = _dot(x1[...], w[...])
        if rot:
            for h in range(w.shape[1] // HEAD):
                c = slice(h * HEAD, (h + 1) * HEAD)
                x = y[:, c]
                dst[:, c] = (x * cs_ref[...] + pltpu.roll(x, HEAD // 2, 1) * sn_ref[...]).astype(BF)
        else:
            dst[...] = y.astype(BF)
    for h in range(qs.shape[1] // HEAD):
        c = slice(h * HEAD, (h + 1) * HEAD)
        for i in range(s // QB):
            n = (i + 1) * QB
            sc = _dot_t(qs[i * QB:n, c], ks[0:n, c])
            d = sc[:, i * QB:]
            low = lax.broadcasted_iota(jnp.int32, (QB, QB), 0) >= lax.broadcasted_iota(jnp.int32, (QB, QB), 1)
            d = jnp.where(low, d, -1e30)
            sc = jnp.concatenate([sc[:, :i * QB], d], axis=1) if i else d
            m = jnp.max(sc, axis=-1, keepdims=True)
            p = jnp.exp((sc - m) * HEAD ** -0.5)
            p = (p * (1.0 / jnp.sum(p, axis=-1, keepdims=True))).astype(BF)
            o_ref[i * QB:n, c] = _dot(p, vs[0:n, c]).astype(BF)

def _attn(h, ln, cs, sn, wq, wk, wv, part, deps=()):
    s, d = h.shape
    e = wq.shape[1] // 2
    nb = 256
    whole = lambda a: pl.BlockSpec(a.shape, lambda i: (0,) * a.ndim)
    col = pl.BlockSpec((d, nb), lambda i: (0, i + part * (e // nb)))
    return pl.pallas_call(
        _attn_kernel, grid=(e // nb,),
        out_shape=jax.ShapeDtypeStruct((s, e), BF),
        in_specs=[whole(h), whole(ln), whole(cs), whole(sn), col, col, col] + [ANY] * len(deps),
        out_specs=pl.BlockSpec((s, nb), lambda i: (0, i)),
        scratch_shapes=[pltpu.VMEM((s, d), BF)] + [pltpu.VMEM((s, nb), BF)] * 3,
        compiler_params=pltpu.CompilerParams(vmem_limit_bytes=64000000, dimension_semantics=("arbitrary",)),
        cost_estimate=pl.CostEstimate(flops=6 * s * d * e + 4 * s * s * e, bytes_accessed=6 * d * e + 4 * s * d, transcendentals=0),
        name="attention",
    )(h, ln, cs, sn, wq, wk, wv, *deps)

def _proj_kernel(h_ref, oa_ref, ob_ref, ln_ref, wo_ref, *rest):
    a_ref, x2_ref, a = rest[-3:]
    i = pl.program_id(0)
    nb = wo_ref.shape[1]
    c = pl.ds(pl.multiple_of(i * nb, nb), nb)
    k = oa_ref.shape[1]
    o = _dot(oa_ref[...], wo_ref[:k, :]) + _dot(ob_ref[...], wo_ref[k:, :])
    y = (h_ref[:, c].astype(F32) + o).astype(BF)
    a[:, c] = y
    a_ref[...] = y
    @pl.when(i == pl.num_programs(0) - 1)
    def _():
        @pl.loop(0, a.shape[0] // 128)
        def _(j):
            q = pl.ds(pl.multiple_of(j * 128, 128), 128)
            x2_ref[q, :] = _norm(a[q, :], ln_ref[...])

def _proj(h, oa, ob, ln, wo, deps=()):
    s, d = h.shape
    nb = 512
    whole = lambda a: pl.BlockSpec(a.shape, lambda i: (0,) * a.ndim)
    return pl.pallas_call(
        _proj_kernel, grid=(d // nb,),
        out_shape=[jax.ShapeDtypeStruct((s, d), BF)] * 2,
        in_specs=[whole(h), whole(oa), whole(ob), whole(ln), pl.BlockSpec((d, nb), lambda i: (0, i))] + [ANY] * len(deps),
        out_specs=[pl.BlockSpec((s, nb), lambda i: (0, i)), pl.BlockSpec((s, d), lambda i: (0, 0))],
        scratch_shapes=[pltpu.VMEM((s, d), BF)],
        compiler_params=pltpu.CompilerParams(vmem_limit_bytes=64000000, dimension_semantics=("arbitrary",)),
        cost_estimate=pl.CostEstimate(flops=2 * s * d * d, bytes_accessed=2 * d * d + 8 * s * d, transcendentals=0),
        name="projection",
    )(h, oa, ob, ln, wo, *deps)

def _ffn_kernel(n2, a_ref, x2, w1_ref, w3_ref, w2_ref, *rest):
    out_ref, sb = rest[-2:]
    i = pl.program_id(0)
    fb = w1_ref.shape[1]
    @pl.when(i < n2)
    def _():
        g = _dot(x2[...], w1_ref[...])
        v = _dot(x2[...], w3_ref[...])
        sb[:, pl.ds(pl.multiple_of(i * fb, fb), fb)] = (g * jax.nn.sigmoid(g) * v).astype(BF)
    @pl.when(i >= n2)
    def _():
        out_ref[...] = a_ref[...].astype(F32) + _dot(sb[...], w2_ref[...])

def _ffn(a, x2, w1, w3, w2, deps=()):
    s, d = a.shape
    f = w1.shape[1]
    nb, fb = 512, 256
    n2, n3 = f // fb, d // nb
    step = lambda i: (0, jnp.clip(i - n2, 0, n3 - 1))
    wide = lambda i: (0, jnp.minimum(i, n2 - 1))
    return pl.pallas_call(
        functools.partial(_ffn_kernel, n2), grid=(n2 + n3,),
        out_shape=jax.ShapeDtypeStruct((s, d), F32),
        in_specs=[pl.BlockSpec((s, nb), step), pl.BlockSpec((s, d), lambda i: (0, 0)),
                  pl.BlockSpec((d, fb), wide), pl.BlockSpec((d, fb), wide), pl.BlockSpec((f, nb), step)] + [ANY] * len(deps),
        out_specs=pl.BlockSpec((s, nb), step),
        scratch_shapes=[pltpu.VMEM((s, f), BF)],
        compiler_params=pltpu.CompilerParams(vmem_limit_bytes=64000000, dimension_semantics=("arbitrary",)),
        cost_estimate=pl.CostEstimate(flops=6 * s * d * f, bytes_accessed=6 * d * f + 8 * s * d, transcendentals=0),
        name="ffn",
    )(a, x2, w1, w3, w2, *deps)

def _angles(s):
    half = HEAD // 2
    freq = 10000.0 ** (-jnp.arange(half, dtype=F32) / half)
    ang = jnp.arange(s, dtype=F32)[:, None] * freq[None, :]
    c, sn = jnp.cos(ang), jnp.sin(ang)
    return jnp.concatenate([c, c], axis=1), jnp.concatenate([-sn, sn], axis=1)


T, D, FE, EL, CAP, NR = 1024, 2048, 1408, 4, 192, 768
MB = 1024

def _tables(meta, base, tab_ref):
    ps, gt = meta[0:8], meta[8:16]
    rows = [[], [], [], []]
    for e in range(EL):
        lo = ((base + e) * CAP).astype(F32)
        hit = (ps >= lo) & (ps < lo + CAP)
        s = jnp.sum(jnp.where(hit, ps - lo + 1.0, 0.0), axis=0, keepdims=True) - 1.0
        g = jnp.sum(jnp.where(hit, gt, 0.0), axis=0, keepdims=True)
        hi = g.astype(BF).astype(F32)
        r = g - hi
        mid = r.astype(BF).astype(F32)
        lo = r - mid
        for lst, v in zip(rows, (s, hi, mid, lo)): lst.append(v)
    tab_ref[...] = jnp.concatenate(sum(rows, []), axis=0)

def _select_block(tt, cb, q, o0):
    n = tt.shape[0]
    for e2 in range(2):
        k = (lax.broadcasted_iota(jnp.int32, (n, 2 * CAP), 1)).astype(F32)
        ea, eb = 2 * e2, 2 * e2 + 1
        ha = k == tt[:, ea:ea + 1]
        hb = k == jnp.where(tt[:, eb:eb + 1] >= 0.0, tt[:, eb:eb + 1] + float(CAP), -1.0)
        for part in range(3):
            o = 4 * (part + 1)
            cc = jnp.where(ha, tt[:, o + ea:o + ea + 1], jnp.where(hb, tt[:, o + eb:o + eb + 1], 0.0))
            c0 = o0 + part * NR + e2 * 2 * CAP
            cb[q, c0:c0 + 2 * CAP] = cc.astype(BF)

def _columns(tab):
    return jnp.concatenate([tab, jnp.zeros((112, T), F32)], axis=0).T

ROWS, SUMS = range(2)

def _experts_kernel(nc, up_n, mode, base_ref, m0_ref, m1_ref, u0a, u0b, u1a, u1b, w1, w3, w2, *rest):
    ub, xy, b1, b3, b2, hb, cb, tab, tabt, stg, usem, wsem, osem, rsem = rest[-14:]
    outs = rest[-14 - (2, 3)[mode]:-14]
    base = base_ref[0]
    wide = 1024
    def wcopies(e, slot):
        return [pltpu.make_async_copy(s.at[e], d.at[slot], wsem.at[i, slot]) for i, (s, d) in enumerate(((w1, b1), (w3, b3)))]
    def dcopy(e):
        return pltpu.make_async_copy(w2.at[e], b2, wsem.at[2, 0])
    def ycopies(e):
        return [pltpu.make_async_copy(xy.at[pl.ds(pl.multiple_of((2 * e + g) * CAP, CAP), CAP)], p.at[pl.ds(pl.multiple_of(e * CAP, CAP), CAP)], rsem.at[g]) for g, p in enumerate(outs[:(2, 0)[mode]])]
    ucs = [[pltpu.make_async_copy(u, ub.at[i, j * T // 2:(j + 1) * T // 2], usem.at[i, j]) for j, u in enumerate(us)] for i, us in enumerate(((u0a, u0b), (u1a, u1b)))]
    for c in ucs[0] + ucs[1]: c.start()
    for g, m in enumerate((m0_ref, m1_ref)):
        _tables(m[...], base, tab.at[g])
    for g in range(2):
        it = lax.broadcasted_iota(jnp.int32, (CAP, T), 0).astype(F32)
        for e in range(EL):
            hit = it == tab[g, e:e + 1, :]
            cb[0, e * CAP:(e + 1) * CAP, g * T:(g + 1) * T] = jnp.where(hit, 1.0, 0.0).astype(BF)
        if mode != ROWS:
            tabt[g] = _columns(tab[g])
    for g in range(2):
        for c in ucs[g]: c.wait()
        if g == 0:
            for c in wcopies(0, 0): c.start()
        else:
            dcopy(0).start()
            for c in wcopies(1, 1): c.start()
        @pl.loop(0, D // wide)
        def _(n):
            c = pl.ds(pl.multiple_of(n * wide, wide), wide)
            x = _dot(cb[0, 0:NR, g * T:(g + 1) * T], ub[g, :, c]).astype(BF)
            for e in range(EL):
                xy[pl.ds(e * 2 * CAP + g * CAP, CAP), c] = x[e * CAP:(e + 1) * CAP]
    @pl.loop(0, EL)
    def _(e):
        slot = lax.rem(e, 2)
        cs = wcopies(e, slot)
        cs[0].wait(); cs[1].wait()
        r = pl.ds(pl.multiple_of(e * 2 * CAP, 2 * CAP), 2 * CAP)
        if up_n == 0:
            g_ = _dot(xy[r, :], b1[slot]); v_ = _dot(xy[r, :], b3[slot])
            hb[...] = (g_ * jax.nn.sigmoid(g_) * v_).astype(BF)
        else:
            for n0 in range(0, FE // 256 * 256, up_n):
                k = min(up_n, FE // 256 * 256 - n0)
                g_ = _dot(xy[r, :], b1[slot, :, n0:n0 + k]); v_ = _dot(xy[r, :], b3[slot, :, n0:n0 + k])
                hb[:, n0:n0 + k] = (g_ * jax.nn.sigmoid(g_) * v_).astype(BF)
                if mode != ROWS and n0 // up_n < 4:
                    q = pl.ds(pl.multiple_of(lax.rem(e, 2) * 512 + n0 // up_n * 128, 128), 128)
                    _select_block(tabt[e // 2, q, :], cb.at[e // 2], q, 0)
            n0 = FE // 256 * 256
            w = jnp.concatenate([b1[slot, :, n0:], b3[slot, :, n0:]], axis=1)
            gv = _dot(xy[r, :], w)
            g_, v_ = gv[:, :FE - n0], gv[:, FE - n0:]
            hb[:, n0:] = (g_ * jax.nn.sigmoid(g_) * v_).astype(BF)
        @pl.when(e + 2 < EL)
        def _():
            for c in wcopies(e + 2, slot): c.start()
        dcopy(e).wait()
        @pl.loop(0, D // wide)
        def _(n):
            c = pl.ds(pl.multiple_of(n * wide, wide), wide)
            xy[r, c] = _dot(hb[...], b2[:, c]).astype(BF)
        @pl.when(e + 1 < EL)
        def _():
            dcopy(e + 1).start()
        for c in ycopies(e): c.start()
    steps = D // nc
    def combine(g, p, first, steps):
        def oc(n): return pltpu.make_async_copy(stg.at[lax.rem(n, 2)], p.at[:, pl.ds(pl.multiple_of(n * nc, nc), nc)], osem.at[lax.rem(n, 2)])
        @pl.loop(0, steps)
        def _(n):
            c = pl.ds(pl.multiple_of((n + first) * nc, nc), nc)
            y = jnp.concatenate([xy[e * 2 * CAP + g * CAP:e * 2 * CAP + (g + 1) * CAP, c] for e in range(EL)], axis=0)
            @pl.when(n >= 2)
            def _(): oc(n - 2).wait()
            y3 = jnp.concatenate([y, y, y], axis=0)
            for mb in range(0, T, MB):
                stg[lax.rem(n, 2), mb:mb + MB] = _dot(cb[g, mb:mb + MB, :], y3)
            oc(n).start()
        oc(steps - 2).wait(); oc(steps - 1).wait()
    if mode == ROWS:
        @pl.loop(0, EL)
        def _(e):
            for c in ycopies(e): c.wait()
        return
    combine(0, outs[0], 0, steps)
    combine(1, outs[1], 0, steps // 2)
    combine(1, outs[2], steps // 2, steps // 2)

def _experts(base, m0, m1, u0, u1, w1, w3, w2, deps=(), mode=SUMS, nc=512, up_n=256):
    row, half = jax.ShapeDtypeStruct((NR, D), BF), jax.ShapeDtypeStruct((T, D // 2), F32)
    shapes = [row] * 2 if mode == ROWS else [jax.ShapeDtypeStruct((T, D), F32), half, half]
    anys = pl.BlockSpec(memory_space=pl.ANY)
    vm = pl.BlockSpec(memory_space=pltpu.VMEM)
    fl = 2 * 2 * (NR * T * D + NR * D * FE * 3 + 3 * mode * T * NR * D)
    return pl.pallas_call(
        functools.partial(_experts_kernel, nc, up_n, mode),
        out_shape=shapes,
        in_specs=[pl.BlockSpec(memory_space=pltpu.SMEM), vm, vm] + [anys] * (7 + len(deps)),
        out_specs=[anys] * len(shapes),
        scratch_shapes=[
            pltpu.VMEM((2, T, D), BF), pltpu.VMEM((2 * NR, D), BF),
            pltpu.VMEM((2, D, FE), BF), pltpu.VMEM((2, D, FE), BF), pltpu.VMEM((FE, D), BF),
            pltpu.VMEM((2 * CAP, FE), BF), pltpu.VMEM((1 if mode == ROWS else 2, T, 3 * NR), BF),
            pltpu.VMEM((2, 16, T), F32), pltpu.VMEM((2, T, 128), F32),
            pltpu.VMEM((2, T, nc), F32),
            pltpu.SemaphoreType.DMA((2, 2)), pltpu.SemaphoreType.DMA((3, 2)), pltpu.SemaphoreType.DMA((2,)), pltpu.SemaphoreType.DMA((2,)),
        ],
        compiler_params=pltpu.CompilerParams(vmem_limit_bytes=67043328),
        cost_estimate=pl.CostEstimate(flops=fl, bytes_accessed=120_000_000, transcendentals=0),
    )(base, m0, m1, *u0, *u1, w1, w3, w2, *deps)

def _prep_kernel(base_ref, m_ref, *rest):
    out, tab, tabt = rest[-3:]
    _tables(m_ref[...], base_ref[pl.program_id(0)], tab)
    tabt[...] = _columns(tab[...])
    @pl.loop(0, T // 128)
    def _(i):
        q = pl.ds(pl.multiple_of(i * 128, 128), 128)
        _select_block(tabt[q, :], out, q, 0)

def _prep(bases, m, deps=()):
    return pl.pallas_call(
        _prep_kernel, grid=(2,),
        out_shape=jax.ShapeDtypeStruct((T, 6 * NR), BF),
        in_specs=[pl.BlockSpec(memory_space=pltpu.SMEM), pl.BlockSpec((16, T), lambda n: (0, 0))] + [pl.BlockSpec(memory_space=pl.ANY)] * len(deps),
        out_specs=pl.BlockSpec((T, 3 * NR), lambda n: (0, n)),
        scratch_shapes=[pltpu.VMEM((16, T), F32), pltpu.VMEM((T, 128), F32)],
        compiler_params=pltpu.CompilerParams(vmem_limit_bytes=64000000, dimension_semantics=("arbitrary",)),
        cost_estimate=pl.CostEstimate(flops=12 * T * NR * 200, bytes_accessed=12 * T * NR, transcendentals=0),
        name="gather_gates",
    )(bases, m, *deps)

def _gather_kernel(na, no, nc, cb, ya, yb, *rest):
    adds, halves, outs = rest[:na], rest[na:na + 2], rest[-no:]
    n = pl.program_id(0)
    y = jnp.concatenate([ya[...]] * 3 + [yb[...]] * 3, axis=0)
    per = D // nc // no
    for mb in range(0, T, MB):
        q = slice(mb, mb + MB)
        acc = _dot(cb[q, :], y)
        for a in adds: acc = acc + a[q, :]
        acc = acc + jnp.where(2 * n < D // nc, halves[0][q, :], halves[1][q, :])
        for j, o in enumerate(outs):
            if no == 1:
                o[q, :] = acc
            else:
                @pl.when(n // per == j)
                def _(o=o): o[q, :] = acc

def _gather(cb, ya, yb, adds, halves, no=1, deps=(), nc=512):
    anys = pl.BlockSpec(memory_space=pl.ANY)
    per = D // nc // no
    half = D // nc // 2
    blk = pl.BlockSpec((T, nc), lambda n: (0, n))
    row = pl.BlockSpec((NR, nc), lambda n: (0, n))
    return pl.pallas_call(
        functools.partial(_gather_kernel, len(adds), no, nc), grid=(D // nc,),
        out_shape=[jax.ShapeDtypeStruct((T, D // no), F32)] * no,
        in_specs=[pl.BlockSpec((T, 6 * NR), lambda n: (0, 0)), row, row] + [blk] * len(adds)
        + [pl.BlockSpec((T, nc), lambda n, j=j: (0, jnp.clip(n - j * half, 0, half - 1))) for j in range(2)] + [anys] * len(deps),
        out_specs=[pl.BlockSpec((T, nc), lambda n, j=j: (0, jnp.clip(n - j * per, 0, per - 1))) for j in range(no)],
        compiler_params=pltpu.CompilerParams(vmem_limit_bytes=64000000, dimension_semantics=("arbitrary",)),
        cost_estimate=pl.CostEstimate(flops=12 * T * NR * D, bytes_accessed=4 * NR * D + 4 * T * D * (1 + len(adds)), transcendentals=0),
        name="gather_rows",
    )(cb, ya, yb, *adds, *halves, *deps)


def _sum_kernel(n, *refs):
    acc = refs[0][...]
    for r in refs[1:n]:
        acc = acc + r[...]
    refs[-1][...] = acc.astype(refs[-1].dtype)


def _sum(parts, dtype, width, deps=(), into=None):
    s = parts[0][0].shape[0]
    rb = 256
    spec = lambda c: pl.BlockSpec((rb, width), lambda i, c=c: (i, c))
    extra = list(deps) + ([into[0]] if into and into[0] is not None else [])
    alias = {len(parts) + len(deps): 0} if into and into[0] is not None else {}
    return pl.pallas_call(
        functools.partial(_sum_kernel, len(parts)), grid=(s // rb,),
        out_shape=jax.ShapeDtypeStruct((s, into[2] if into else width), dtype),
        in_specs=[spec(c) for _, c in parts] + [ANY] * len(extra),
        out_specs=spec(into[1] if into else 0),
        input_output_aliases=alias,
        compiler_params=pltpu.CompilerParams(dimension_semantics=("arbitrary",)),
        cost_estimate=pl.CostEstimate(flops=3 * s * width * 1000, bytes_accessed=16 * s * width, transcendentals=0),
        name="ring_sum",
    )(*[a for a, _ in parts], *extra)

def _gate(u, wr, gi):
    lg = jnp.einsum('td,de->te', u, wr, preferred_element_type=F32)
    hit = gi[..., None] == jnp.arange(wr.shape[1], dtype=gi.dtype)
    return jax.nn.softmax(jnp.sum(jnp.where(hit, lg[:, None, :], 0.0), axis=-1), axis=-1)


CYCLE = [(0, 0), (1, 0), (2, 0), (3, 0), (3, 1), (2, 1), (1, 1), (0, 1)]
DEV = [[(z * 2 + y) * 2 + c for c in range(2)] for z, y in CYCLE]


def _perm(step, cross):
    n = len(CYCLE)
    sign = (-1, 1) if cross else (1, -1)
    return [(DEV[p][c], DEV[(p + sign[c] * step) % n][1 - c if cross else c]) for p in range(n) for c in range(2)]


def _from(step, el):
    n = len(CYCLE)
    t = np.zeros((2 * n, 2), np.int32)
    for p in range(n):
        for c in range(2):
            q = (p - (1, -1)[c] * step) % n
            t[DEV[p][c]] = (DEV[q][c] * el, DEV[q][1 - c] * el)
    return t


def solution(mesh):
    g_ = mesh.shape['ep']
    assert g_ == 2 * len(CYCLE)
    rows = P(('dp', 'ep'))
    rep = P()
    ahead, behind, swap_p = _perm(1, False), _perm(-1, False), _perm(0, True)

    def send(x, perm):
        return jax.tree.map(lambda t: lax.ppermute(t, 'ep', perm), x)

    def local(h0, idx, slot, ln_attn, wq, wk, wv, wo, ln_ffn, ws1, ws3, ws2, ln_moe, wr, ue1, ue3, ue2):
        bb, s, d = h0.shape
        top = idx.shape[-1]
        el = ue1.shape[0]
        assert (bb, s, d) == (1, T, D) and ue1.shape == (EL, D, FE) and top <= 8
        h = h0.reshape(s, d)
        ha, hb = h[:s // 2], h[s // 2:]
        ua = _norm(ha, ln_moe)
        hb, ua = lax.optimization_barrier((hb, ua))
        u = ua, _norm(hb, ln_moe)
        gi = idx.reshape(s, top)
        gate = jnp.concatenate([_gate(v, wr, x) for v, x in zip(u, (gi[:s // 2], gi[s // 2:]))])

        def pad(x, v):
            return jnp.pad(x.astype(F32).T, ((0, 8 - top), (0, 0)), constant_values=v)

        meta = jnp.concatenate([pad(gi * CAP + slot.reshape(s, top), -1.0), pad(gate, 0.0)], axis=0)
        me = lax.axis_index('ep')
        base = (me * el).astype(jnp.int32).reshape(1)
        base_up = jnp.asarray(_from(1, el))[me]
        base_down = jnp.asarray(_from(-1, el))[me]
        width = d // NRING

        def experts(x, y, *deps):
            mine, *theirs = _experts(base, x[1], y[1], x[0], y[0], ue1, ue3, ue2, deps)
            return mine, send(theirs, swap_p)

        def rows_of(x, y, *deps):
            return _experts(base, x[1], y[1], x[0], y[0], ue1, ue3, ue2, deps, mode=ROWS)

        def add(i, run, pair, dep):
            part = _sum([(run[i], 0), (pair[0], i), (pair[1][i], 0)], F32, width, (dep,))
            run[i] = send(part, ahead)
            return part

        def gates(bases, m, *deps):
            return _prep(bases, m, deps)

        own = (u, meta)
        own_o = send(own, swap_p)

        def hop(x, perm, after):
            out = []
            for i in range(2):
                v = lax.optimization_barrier((x[0][i], after[i]))[0] if after else x[0][i]
                out.append(send(v, perm))
            return tuple(out), send(x[1], perm)

        f0, b0 = hop(own, ahead, None), hop(own, behind, None)
        angles = _angles(s)
        oa = _attn(h, ln_attn[None], *angles, wq, wk, wv, 0, u)
        ob = _attn(h, ln_attn[None], *angles, wq, wk, wv, 1, (oa,))
        f1, b1 = hop(f0, ahead, (oa, ob)), hop(b0, behind, (oa, ob))
        p6 = experts(b0, send(b0, swap_p), ob)
        a, x2 = _proj(h, oa, ob, ln_ffn[None], wo, (p6[0],))
        f2, b2 = hop(f1, ahead, (p6[0], a)), hop(b1, behind, (p6[0], a))
        r1 = rows_of(f1, send(f1, swap_p), a)
        chain = send(r1[0], ahead), send(r1[1], _perm(1, True))
        r0 = rows_of(f0, send(f0, swap_p), r1[0])
        f3 = hop(f2, ahead, (r0[0], r0[0]))
        p2 = experts(f2, send(f2, swap_p), r0[0])
        r00, r01, p20 = lax.optimization_barrier((*r0, p2[0]))
        direct = send(r00, behind), send(r01, _perm(-1, True))
        g2 = gates(base_up, f2[1], p20)
        q = _gather(g2, *chain, p2[:1], p2[1], NRING)
        run = [send(x, ahead) for x in q]
        p3 = experts(f3, send(f3, swap_p), q[0])
        g7 = gates(base_down, meta, p3[0])
        r = add(0, run, p3, g7)
        p4 = experts(b2, send(b2, swap_p), r)
        r = add(1, run, p3, p4[0])
        r = add(0, run, p4, r)
        p5 = experts(b1, send(b1, swap_p), r)
        r = add(1, run, p4, p5[0])
        r = add(0, run, p5, r)
        p7 = experts(own, own_o, r)
        r = add(1, run, p5, p7[0])
        r = add(0, run, p6, r)
        base_sum, = _gather(g7, *direct, p7[:1], p7[1], 1, (r,))
        r = add(1, run, p6, base_sum)
        af = _ffn(a, x2, ws1, ws3, ws2, (r,))
        out = None
        for i in range(NRING):
            out = _sum([(af, i), (base_sum, i), (run[i], 0)], jnp.bfloat16, width, (), (out, i, d))
        return out.reshape(bb, s, d)

    specs = (rows, rows, rows) + (rep,) * 11 + (P('ep'), P('ep'), P('ep'))
    return jax.shard_map(local, mesh=mesh, in_specs=specs, out_specs=rows, check_vma=False)
```
